32 devices in a mesh: shard: 8 (over y, x, core), width: 4 (over z).
Axes of the slice: x: 2, y: 2, z: 4, core: 2. Of those that a mesh axis runs over, the one named last changes fastest.
Arguments:
- w_up: bfloat16 [12288, 49152], P('shard', 'width'), may hold values from -0.078125 to 0.078125
- low_up: bfloat16 [12288, 64], P('shard'), may hold values from -0.0546875 to 0.0546875
- high_up: bfloat16 [64, 49152], P(None, 'width'), may hold values from -0.75 to 0.75
- norm_train: float32 [12288], P(('shard', 'width')), may hold values from 0.25 to 1.75
- norm_step: float32 [12288], P(('shard', 'width')), may hold values from -0.3 to 0.3
Outputs:
- serve_up: bfloat16 [12288, 49152], P(None, ('width', 'shard'))
- scale_up: float32 [49152], P(('width', 'shard'))
- serve_norm: bfloat16 [12288], replicated
The draws below stay inside these ranges and needn't reach their ends.
All inputs are finite; a program needn't handle non-finite values. Where the reference program divides by a largest or mean magnitude, that divisor is 1e-20 or more.
Results may differ from the reference program's by a relative error of at most 0.001.
Values may be sent and summed in bfloat16 or wider, within the bound.
A program may use at most 256 MiB of HBM per device.

```python
import jax
import jax.numpy as jnp

D_MODEL = 12288
D_INNER = 49152
RANK = 64


def raised(drawn, own_key, source, target, blocks, factor):
    def block_of(dim):
        return (jnp.arange(drawn.shape[dim]) // (drawn.shape[dim] // blocks)).reshape((-1,) + (1,) * (drawn.ndim - 1 - dim))

    one_side = jax.random.permutation(own_key, blocks)[block_of(target)]
    far = (block_of(target) + blocks // 2) % blocks
    return jnp.where((block_of(source) == one_side) | (block_of(source) == far), factor * drawn, drawn)


def block_levels(rng, extent, shards, smallest, high):
    def one(dim, parts):
        draws = jax.random.uniform(jax.random.fold_in(jax.random.fold_in(rng, 6), dim), (parts,), jnp.float32, smallest / len(shards), high / len(shards))
        return jnp.repeat(jnp.exp(draws), extent[dim] // parts).reshape((-1,) + (1,) * (len(extent) - dim - 1))

    gain = one(*shards[0])
    for cut in shards[1:]:
        gain = gain * one(*cut)
    return gain


def gaussian(rng, dims, width, reach, split=(), held_as=jnp.bfloat16):
    entries = width * jax.random.normal(rng, dims, jnp.float32)
    if split:
        entries = entries * block_levels(rng, dims, split, -0.22, 0.18)
    return jnp.clip(entries, -reach, reach).astype(held_as)


def heavy_noise(rng, extent, deviation, bound, cuts, heavy, held_as=jnp.bfloat16):
    result = deviation * jax.random.normal(rng, extent, jnp.float32)
    if cuts:
        result = result * block_levels(rng, extent, cuts, -0.22, 0.18)
    return jnp.clip(raised(result, jax.random.fold_in(rng, 3), *heavy), -bound, bound).astype(held_as)


def setup_inputs(seed: int = 0) -> dict:
    key_of = jax.random.split(jax.random.key(seed), 6)
    w_up = heavy_noise(key_of[0], (D_MODEL, D_INNER), D_MODEL ** -0.5, 0.078125, ((0, 8), (1, 4)), (0, 1, 8, 2.0))
    low_up = gaussian(key_of[1], (D_MODEL, RANK), D_MODEL ** -0.5, 0.0546875, ((0, 8),))
    high_up = gaussian(key_of[2], (RANK, D_INNER), RANK ** -0.5, 0.75, ((1, 4),))
    norm_train = jnp.clip(1.0 + 0.15 * jax.random.normal(key_of[3], (D_MODEL,), jnp.float32), 0.25, 1.75)
    norm_step = jnp.clip(jax.random.uniform(key_of[4], (D_MODEL,), jnp.float32, -0.3, 0.3) * block_levels(key_of[4], (D_MODEL,), ((0, 32),), -0.4, 0.0), -0.3, 0.3)
    return dict(w_up=w_up, low_up=low_up, high_up=high_up, norm_train=norm_train, norm_step=norm_step)


mix_rate = 0.5


def reference(w_up, low_up, high_up, norm_train, norm_step):
    fresh_up = w_up.astype(jnp.float32) + mix_rate * jnp.dot(low_up, high_up, preferred_element_type=jnp.float32)
    scale_up = jnp.sum(jnp.abs(fresh_up), axis=0) / D_MODEL
    serve_up = (fresh_up / scale_up).astype(jnp.bfloat16)
    serve_norm = (norm_train + norm_step).astype(jnp.bfloat16)
    return serve_up, scale_up, serve_norm
```

```python
import functools

import jax
import jax.numpy as jnp
from jax import lax
from jax.experimental import pallas as pl
from jax.experimental.pallas import tpu as pltpu
from jax.sharding import PartitionSpec as P

MESH = pl.DeviceIdType.MESH

mix_rate = 0.5


def tile_of(extent, most):
    for size in range(most, 0, -128):
        if extent % size == 0:
            return size
    return extent


def contract_first(a, b):
    return lax.dot_general(a, b, (((0,), (0,)), ((), ())), preferred_element_type=jnp.float32)


def exchange_kernel(
    n, depth, w_ref, low_ref, high_ref, small_ref,
    g_ref, all_ref, mine_ref, parts_ref,
    send_sem, recv_sem, small_send, small_recv, far_send, far_recv, part_send, part_recv, own_sem,
):
    me = lax.axis_index("shard")
    z = lax.axis_index("width")
    rows = w_ref.shape[0]
    rank = low_ref.shape[0]
    cols = g_ref.shape[1]
    order = sorted(range(1, n), key=lambda k: (bin(k >> 1).count("1"), k))

    def columns(p):
        return pl.ds(pl.multiple_of(p * cols, cols), cols)

    def rows_of(p):
        return pl.ds(pl.multiple_of(p * rows, rows), rows)

    def small_copy(k):
        return pltpu.make_async_remote_copy(
            src_ref=small_ref, dst_ref=all_ref.at[me, z],
            send_sem=small_send.at[k], recv_sem=small_recv.at[k],
            device_id={"shard": me ^ k}, device_id_type=MESH,
        )

    def big_copy(k):
        return pltpu.make_async_remote_copy(
            src_ref=w_ref.at[:, columns(me ^ k)], dst_ref=g_ref.at[rows_of(me), :],
            send_sem=send_sem.at[k], recv_sem=recv_sem.at[k],
            device_id={"shard": me ^ k}, device_id_type=MESH,
        )

    def part_copy(k):
        return pltpu.make_async_remote_copy(
            src_ref=mine_ref.at[:, columns(me ^ k)], dst_ref=parts_ref.at[me],
            send_sem=part_send.at[k], recv_sem=part_recv.at[k],
            device_id={"shard": me ^ k}, device_id_type=MESH,
        )

    def far_copy(k):
        return pltpu.make_async_remote_copy(
            src_ref=all_ref.at[:, z], dst_ref=all_ref.at[:, z],
            send_sem=far_send.at[k], recv_sem=far_recv.at[k],
            device_id={"width": z ^ k}, device_id_type=MESH,
        )

    own_small = pltpu.make_async_copy(small_ref, all_ref.at[me, z], own_sem.at[0])
    own_small.start()
    for k in order:
        small_copy(k).start()
    for k in order:
        big_copy(k).start()

    own_small.wait()
    for k in order:
        small_copy(k).wait()
    for k in range(1, depth):
        far_copy(k).start()

    tile = tile_of(w_ref.shape[1], 512)
    step = tile_of(rows, 256)

    def add_up(w_tile, high_tile, sum_tile):
        total = jnp.zeros((8, tile), jnp.float32)
        for r in range(0, rows, step):
            fresh = w_tile[r:r + step, :].astype(jnp.float32) + mix_rate * contract_first(
                low_ref[:, r:r + step], high_tile[...]
            )
            total = total + jnp.sum(jnp.abs(fresh).reshape(step // 8, 8, tile), axis=0)
        sum_tile[...] = jnp.sum(total, axis=0, keepdims=True)

    pltpu.emit_pipeline(
        add_up,
        grid=(w_ref.shape[1] // tile,),
        in_specs=[
            pl.BlockSpec((rows, tile), lambda j: (0, j)),
            pl.BlockSpec((rank, tile), lambda j: (0, j)),
        ],
        out_specs=[pl.BlockSpec((1, tile), lambda j: (0, j))],
    )(w_ref, high_ref, mine_ref)

    own_part = pltpu.make_async_copy(mine_ref.at[:, columns(me)], parts_ref.at[me], own_sem.at[1])
    own_part.start()
    for k in order:
        part_copy(k).start()

    band = tile_of(rows, 384)

    def take_over(source, target):
        target[...] = source[...]

    pltpu.emit_pipeline(
        take_over,
        grid=(rows // band,),
        in_specs=[pl.BlockSpec((band, cols), lambda i: (i, me))],
        out_specs=[pl.BlockSpec((band, cols), lambda i: (me * (rows // band) + i, 0))],
    )(w_ref, g_ref)

    own_part.wait()
    for k in range(1, depth):
        far_copy(k).wait()
    for k in order:
        part_copy(k).wait()
    for k in order:
        big_copy(k).wait()


def finish_kernel(inner, w_ref, small_ref, high_ref, parts_ref, out_ref, scale_ref):
    rank = high_ref.shape[0]
    height = w_ref.shape[0]
    scale = jnp.sum(parts_ref[...], axis=0) / inner
    scale_ref[...] = scale
    inverse = 1.0 / scale
    step = tile_of(height, 128)
    for r in range(0, height, step):
        fresh = w_ref[r:r + step, :].astype(jnp.float32) + contract_first(
            small_ref[:rank, r:r + step], high_ref[...]
        )
        out_ref[r:r + step, :] = (fresh * inverse).astype(jnp.bfloat16)


def solution(mesh):
    n, depth = mesh.shape["shard"], mesh.shape["width"]

    def per_device(w_up, low_up, high_up, norm_train, norm_step):
        rows, wide = w_up.shape
        rank = low_up.shape[1]
        cols = wide // n
        part = rows // depth
        me = lax.axis_index("shard")
        z = lax.axis_index("width")
        low = low_up.T
        gain = (norm_train + norm_step).astype(jnp.bfloat16).reshape(1, part)
        small = jnp.concatenate(
            [
                lax.dynamic_slice_in_dim(low, z * part, part, axis=1) * jnp.bfloat16(mix_rate),
                jnp.broadcast_to(gain, (16, part)),
            ],
            axis=0,
        )
        high_own = lax.dynamic_slice_in_dim(high_up, me * cols, cols, axis=1)
        any_spec = pl.BlockSpec(memory_space=pl.ANY)
        dma = pltpu.SemaphoreType.DMA
        gathered, everyone, _, parts = pl.pallas_call(
            functools.partial(exchange_kernel, n, depth),
            out_shape=(
                jax.ShapeDtypeStruct((n * rows, cols), jnp.bfloat16),
                jax.ShapeDtypeStruct((n, depth) + small.shape, jnp.bfloat16),
                jax.ShapeDtypeStruct((1, wide), jnp.float32),
                jax.ShapeDtypeStruct((n, 1, cols), jnp.float32),
            ),
            in_specs=[any_spec, pl.BlockSpec(memory_space=pltpu.VMEM), any_spec, any_spec],
            out_specs=(any_spec,) * 4,
            scratch_shapes=[
                dma((n,)), dma((n,)), dma((n,)), dma((n,)), dma((depth,)), dma((depth,)),
                dma((n,)), dma((n,)), dma((2,)),
            ],
            compiler_params=pltpu.CompilerParams(has_side_effects=True),
            name="exchange",
        )(w_up, low, high_up, small)
        serve_up, scale_up = pl.pallas_call(
            functools.partial(finish_kernel, n * rows),
            grid=(n * depth,),
            out_shape=(
                jax.ShapeDtypeStruct((n * rows, cols), jnp.bfloat16),
                jax.ShapeDtypeStruct((1, cols), jnp.float32),
            ),
            in_specs=[
                pl.BlockSpec((part, cols), lambda i: (i, 0)),
                pl.BlockSpec((None, None) + small.shape, lambda i: (i // depth, i % depth, 0, 0)),
                pl.BlockSpec((rank, cols), lambda i: (0, 0)),
                pl.BlockSpec((n, 1, cols), lambda i: (0, 0, 0)),
            ],
            out_specs=(
                pl.BlockSpec((part, cols), lambda i: (i, 0)),
                pl.BlockSpec((1, cols), lambda i: (0, 0)),
            ),
            compiler_params=pltpu.CompilerParams(dimension_semantics=("arbitrary",)),
            name="finish",
        )(gathered, everyone, high_own, parts)
        serve_norm = everyone[:, :, rank, :].reshape(n * rows)
        return serve_up, scale_up.reshape(cols), serve_norm

    placed = (
        P("shard", "width"),
        P("shard", None),
        P(None, "width"),
        P(("shard", "width")),
        P(("shard", "width")),
    )
    return jax.shard_map(
        per_device,
        mesh=mesh,
        in_specs=placed,
        out_specs=(P(None, ("width", "shard")), P(("width", "shard")), P()),
        check_vma=False,
    )
```
